32 devices in a mesh: shard: 8 (over z, x), model: 4 (over y, core).
Axes of the slice: x: 2, y: 2, z: 4, core: 2. Of those that a mesh axis runs over, the one named last changes fastest.
Arguments:
- grad_stack: float32 [64, 128, 2048], P(None, 'shard', 'model'), may hold values from -6 to 6
- moment_stack: float32 [64, 128, 2048], P(None, 'shard', 'model'), may hold values from -6 to 6
- weight_stack: float32 [64, 128, 2048], P(None, 'shard', 'model'), may hold values from -0.1875 to 0.1875
Outputs:
- new_weights: float32 [64, 128, 2048], P(None, 'shard', 'model')
- new_momentum: float32 [64, 128, 2048], P(None, 'shard', 'model')
The draws below stay inside these ranges and needn't reach their ends.
All inputs are finite; a program needn't handle non-finite values.
Results may differ from the reference program's by a relative error of at most 0.00021.
Values sent between devices are 32-bit elements; how exact they have to be, the bound alone decides.
No kernel may reach another device: no remote copies, remote signals or barrier semaphores. Data moves between devices by JAX's collectives and lax.ppermute only.
A program may use at most 64 MiB of HBM per device.

```python
import jax
import jax.numpy as jnp
from jax import lax

SIDE = 128
WIDE = 2048
MATS = 64
ITERS = 5


def shard_levels(own_key, extent, pieces, least, high):
    def one(position, parts):
        steps = jax.random.uniform(jax.random.fold_in(jax.random.fold_in(own_key, 6), position), (parts,), jnp.float32, least / len(pieces), high / len(pieces))
        return jnp.repeat(jnp.exp(steps), extent[position] // parts).reshape((-1,) + (1,) * (len(extent) - position - 1))

    loudness = one(*pieces[0])
    for cut in pieces[1:]:
        loudness = loudness * one(*cut)
    return loudness


def noise(rng, extent, width, most, shards=(), held_as=jnp.bfloat16):
    drawn = jax.random.normal(rng, extent, jnp.float32) * width
    if len(shards) > 0:
        drawn = shard_levels(rng, extent, shards, -0.22, 0.18) * drawn
    return jnp.clip(drawn, min=-most, max=most).astype(held_as)


def setup_inputs(seed: int = 0) -> dict:
    key_list = jax.random.split(jax.random.key(seed), 4)
    grad_stack = noise(key_list[0], (MATS, SIDE, WIDE), 1.0, 6.0, ((1, 8), (2, 4)), jnp.float32)
    moment_stack = noise(key_list[1], (MATS, SIDE, WIDE), 1.0, 6.0, ((1, 8), (2, 4)), jnp.float32)
    weight_stack = noise(key_list[2], (MATS, SIDE, WIDE), 0.03, 0.1875, ((1, 8), (2, 4)), jnp.float32)
    return {"grad_stack": grad_stack, "moment_stack": moment_stack, "weight_stack": weight_stack}


hold_rate = 0.95
learn_rate = 1.0
decay_rate = 0.1

def reference(grad_stack, moment_stack, weight_stack):
    new_momentum = hold_rate * moment_stack + grad_stack

    def orthogonal_one(stack):
        iterate = stack[None]
        iterate = iterate * lax.rsqrt(lax.optimization_barrier(jnp.sum(iterate * iterate, axis=(1, 2), keepdims=True)) + 1e-06)
        for step in range(ITERS):
            gram = jnp.einsum('mik,mjk->mij', iterate, iterate, precision=lax.Precision.HIGHEST)
            mixed = -4.775 * gram + 2.0315 * jnp.einsum('mij,mjk->mik', gram, gram, precision=lax.Precision.HIGHEST)
            iterate = 3.4445 * iterate + jnp.einsum('mij,mjk->mik', mixed, iterate, precision=lax.Precision.HIGHEST)
        return iterate[0]
    iterate = lax.map(orthogonal_one, new_momentum)
    new_weights = (1.0 - learn_rate * decay_rate) * weight_stack - learn_rate * iterate
    return (new_weights, new_momentum)
```

```python
import jax
import jax.numpy as jnp
from jax import lax
from jax.sharding import PartitionSpec as P

hold_rate = 0.95
learn_rate = 1.0
decay_rate = 0.1
HI = lax.Precision.HIGHEST
A0, A1, A2 = 3.4445, -4.775, 2.0315


def mm(a, b):
    return jnp.einsum("mij,mjk->mik", a, b, precision=HI)


def gram_of(x):
    return jnp.einsum("mik,mjk->mij", x, x, precision=HI)


def factor(g, eye):
    return A0 * eye + A1 * g + A2 * mm(g, g)


def chain(g, steps, eye):
    total = None
    for step in range(steps):
        p = factor(g, eye)
        total = p if total is None else mm(p, total)
        if step < steps - 1:
            g = mm(mm(p, g), p)
    return total


def summed_over_model(g, model):
    half = g.shape[0] // 2
    bit = lax.axis_index("model") % 2
    keep = lax.dynamic_slice_in_dim(g, bit * half, half, 0)
    send = lax.dynamic_slice_in_dim(g, (1 - bit) * half, half, 0)
    own = keep + lax.ppermute(send, "model", [(i, i ^ 1) for i in range(model)])
    dist = 2
    while dist < model:
        own = own + lax.ppermute(own, "model", [(i, i ^ dist) for i in range(model)])
        dist *= 2
    return own


def joined(own, model):
    bit = lax.axis_index("model") % 2
    other = lax.ppermute(own, "model", [(i, i ^ 1) for i in range(model)])
    return jnp.where(bit == 0, jnp.concatenate([own, other]), jnp.concatenate([other, own]))


def process(x, model, first=2, last=3):
    eye = jnp.eye(x.shape[1], dtype=jnp.float32)
    g = summed_over_model(gram_of(x), model)
    r = lax.rsqrt(jnp.einsum("mii->m", g) + 1e-06)[:, None, None]
    q = chain(g * (r * r), first, eye) * r
    x = mm(joined(q, model), x)
    if last:
        g = summed_over_model(gram_of(x), model)
        x = mm(joined(chain(g, last, eye), model), x)
    return x


def make(mesh, K=1, first=2, last=3):
    shards, model = mesh.shape["shard"], mesh.shape["model"]

    def on_device(grad_stack, moment_stack, weight_stack):
        new_momentum = hold_rate * moment_stack + grad_stack
        mats, rows, cols = new_momentum.shape
        x = lax.all_to_all(new_momentum, "shard", split_axis=0, concat_axis=1, tiled=True)
        x = process(x, model, first, last)
        back = lax.all_to_all(x, "shard", split_axis=1, concat_axis=0, tiled=True)
        new_weights = (1.0 - learn_rate * decay_rate) * weight_stack - learn_rate * back
        return (new_weights, new_momentum)
    return on_device


def solution(mesh):
    spec = P(None, "shard", "model")
    return jax.shard_map(
        make(mesh), mesh=mesh, in_specs=(spec,) * 3, out_specs=(spec,) * 2, check_vma=False
    )
```

```python
import jax
import jax.numpy as jnp
from jax import lax
from jax.sharding import PartitionSpec as P


ITERS = 5
hold_rate = 0.95
learn_rate = 1.0
decay_rate = 0.1
HI = lax.Precision.HIGHEST
AXES = ("shard", "model")


def orthogonal(whole):
    norm = lax.rsqrt(jnp.sum(whole * whole, axis=(1, 2), keepdims=True) + 1e-06)
    iterate = whole * norm
    for _ in range(ITERS):
        gram = jnp.einsum("mik,mjk->mij", iterate, iterate, precision=HI)
        mixed = -4.775 * gram + 2.0315 * jnp.einsum("mij,mjk->mik", gram, gram, precision=HI)
        iterate = 3.4445 * iterate + jnp.einsum("mij,mjk->mik", mixed, iterate, precision=HI)
    return iterate


def make(mesh):
    shards, model = mesh.shape["shard"], mesh.shape["model"]
    devices = shards * model

    def on_device(grad_stack, moment_stack, weight_stack):
        new_momentum = hold_rate * moment_stack + grad_stack
        mats, rows, cols = new_momentum.shape
        each = mats // devices
        pieces = 2 if each % 2 == 0 else 1
        w = each // pieces
        split = new_momentum.reshape(devices, each, rows, cols)
        kept = ((1.0 - learn_rate * decay_rate) * weight_stack).reshape(split.shape)
        arrived = []
        for c in range(pieces):
            arrived.append(lax.all_to_all(split[:, c * w:(c + 1) * w], AXES, split_axis=0, concat_axis=0, tiled=True))
        backs = []
        for c in range(pieces):
            x = arrived[c].reshape(shards, model, w, rows, cols).transpose(2, 0, 3, 1, 4)
            x = orthogonal(x.reshape(w, shards * rows, model * cols))
            x = x.reshape(w, shards, rows, model, cols).transpose(1, 3, 0, 2, 4).reshape(devices, w, rows, cols)
            if c + 1 < pieces:
                x, arrived[c + 1] = lax.optimization_barrier((x, arrived[c + 1]))
            backs.append(lax.all_to_all(x, AXES, split_axis=0, concat_axis=0, tiled=True))
        new_weights = kept - learn_rate * jnp.concatenate(backs, axis=1)
        return (new_weights.reshape(mats, rows, cols), new_momentum)

    return on_device


def solution(mesh):
    spec = P(None, "shard", "model")
    return jax.shard_map(
        make(mesh), mesh=mesh, in_specs=(spec,) * 3, out_specs=(spec,) * 2, check_vma=False
    )
```

```python
import functools

import jax
import jax.numpy as jnp
from jax import lax
from jax.experimental import pallas as pl
from jax.experimental.pallas import tpu as pltpu
from jax.sharding import PartitionSpec as P


ITERS = 5
EARLY = 2
hold_rate = 0.95
learn_rate = 1.0
decay_rate = 0.1
A0, A1, A2 = 3.4445, -4.775, 2.0315
HI = lax.Precision.HIGHEST
AXES = ("shard", "model")
F32 = jnp.float32
VMEM = pl.BlockSpec(memory_space=pltpu.VMEM)


def dot(a, b):
    return lax.dot_general(a, b, (((1,), (0,)), ((), ())), precision=HI, preferred_element_type=F32)


def dot_t(a, b):
    return lax.dot_general(a, b, (((1,), (1,)), ((), ())), precision=HI, preferred_element_type=F32)


def eye_of(n):
    i = lax.broadcasted_iota(jnp.int32, (n, n), 0)
    j = lax.broadcasted_iota(jnp.int32, (n, n), 1)
    return (i == j).astype(F32)


def chain(grams, steps, eye):
    totals = None
    for step in range(steps):
        squares = [dot(g, g) for g in grams]
        ps = [A0 * eye + A1 * g + A2 * s for g, s in zip(grams, squares)]
        if step < steps - 1:
            halves = [dot(p, g) for p, g in zip(ps, grams)]
        totals = ps if totals is None else [dot(p, t) for p, t in zip(ps, totals)]
        if step < steps - 1:
            grams = [dot(h, p) for h, p in zip(halves, ps)]
    return totals


def inverse_norm(gram, eye):
    return lax.rsqrt(jnp.sum(gram * eye, axis=(0, 1), keepdims=True) + 1e-06)


def whole_kernel(shards, model, rows, cols, x_ref, o_ref, a_ref):
    eye = eye_of(shards * rows)

    def load(s, _):
        for m in range(model):
            a_ref[pl.ds(pl.multiple_of(s * rows, rows), rows), m * cols:(m + 1) * cols] = x_ref[s * model + m]
        return 0

    lax.fori_loop(0, shards, load, 0)

    def gram(m, total):
        at = pl.ds(pl.multiple_of(m * cols, cols), cols)
        return total + dot_t(a_ref[:, at], a_ref[:, at])

    zero = jnp.zeros(eye.shape, F32)
    g = lax.fori_loop(0, model, gram, zero)
    norm = inverse_norm(g, eye)
    q = chain([g * (norm * norm)], EARLY, eye)[0] * norm

    def early(m, total):
        at = pl.ds(pl.multiple_of(m * cols, cols), cols)
        y = dot(q, a_ref[:, at])
        a_ref[:, at] = y
        return total + dot_t(y, y)

    g = lax.fori_loop(0, model, early, zero)
    r = chain([g], ITERS - EARLY, eye)[0]

    def late(m, _):
        y = dot(r, a_ref[:, pl.ds(pl.multiple_of(m * cols, cols), cols)])
        for s in range(shards):
            o_ref[s * model + m] = y[s * rows:(s + 1) * rows]
        return 0

    lax.fori_loop(0, model, late, 0)


def whole(x, shards, model):
    _, rows, cols = x.shape
    flops = 8 * (shards * rows) ** 2 * model * cols * 6
    return pl.pallas_call(
        functools.partial(whole_kernel, shards, model, rows, cols),
        out_shape=jax.ShapeDtypeStruct(x.shape, F32),
        in_specs=[VMEM],
        out_specs=VMEM,
        scratch_shapes=[pltpu.VMEM((shards * rows, model * cols), F32)],
        cost_estimate=pl.CostEstimate(flops=flops, bytes_accessed=8 * x.size, transcendentals=0),
    )(x)


def mm(a, b):
    return jnp.einsum("mij,mjk->mik", a, b, precision=HI)


def gram_of(x):
    return jnp.einsum("mik,mjk->mij", x, x, precision=HI)


def stacked_chain(g, steps, eye):
    total = None
    for step in range(steps):
        p = A0 * eye + A1 * g + A2 * mm(g, g)
        total = p if total is None else mm(p, total)
        if step < steps - 1:
            g = mm(mm(p, g), p)
    return total


def swap(x, axis, size, bits):
    return lax.ppermute(x, axis, [(i, i ^ bits) for i in range(size)])


def summed(g, model):
    half = g.shape[0] // 2
    bit = lax.axis_index("model") % 2
    own = lax.dynamic_slice_in_dim(g, bit * half, half, 0)
    send = lax.dynamic_slice_in_dim(g, (1 - bit) * half, half, 0)
    own = own + swap(send, "model", model, 1)
    return own + swap(own, "model", model, 2)


def joined(own, model):
    bit = lax.axis_index("model") % 2
    other = swap(own, "model", model, 1)
    return jnp.where(bit == 0, jnp.concatenate([own, other]), jnp.concatenate([other, own]))


def spread(x, model):
    eye = jnp.eye(x.shape[1], dtype=F32)
    g = gram_of(x)
    g = summed(g, model)
    r = lax.rsqrt(jnp.einsum("mii->m", g) + 1e-06)[:, None, None]
    q = stacked_chain(g * (r * r), EARLY, eye) * r
    x = mm(joined(q, model), x)
    g = summed(gram_of(x), model)
    q = joined(stacked_chain(g, ITERS - EARLY, eye), model)
    return mm(q, x)


def direct(blocks, shards):
    return [blocks[0]] + [swap(blocks[d], "shard", shards, d) for d in range(1, shards)]


def mixed(shards, model, grad_stack, moment_stack, weight_stack):
    mats, rows, cols = grad_stack.shape
    each = mats // shards
    w = each // 2
    me = lax.axis_index("shard")
    cut = (shards, each, rows, cols)
    first = hold_rate * moment_stack.reshape(cut)[:, :w] + grad_stack.reshape(cut)[:, :w]
    first, grad_stack = lax.optimization_barrier((first, grad_stack))
    new_momentum = hold_rate * moment_stack + grad_stack
    split = new_momentum.reshape(cut)
    first = lax.all_to_all(first.reshape(shards * model, rows, cols), AXES, split_axis=0, concat_axis=0, tiled=True)
    second = [lax.dynamic_slice(split, (me ^ d, w, 0, 0), (1, w, rows, cols))[0] for d in range(shards)]
    second = direct(second, shards)

    first = whole(first, shards, model)
    first = lax.all_to_all(first, AXES, split_axis=0, concat_axis=0, tiled=True)

    x = jnp.concatenate([b[None] for b in second], axis=0).transpose(1, 0, 2, 3)
    x = spread(x.reshape(w, shards * rows, cols), model).reshape(w, shards, rows, cols)
    second = [x[:, d] for d in range(shards)]
    second = direct(second, shards)

    kept = lax.optimization_barrier((1.0 - learn_rate * decay_rate) * weight_stack.reshape(cut))
    total = kept.at[:, :w].add(-learn_rate * first.reshape(shards, w, rows, cols))
    for d in range(shards):
        at = (me ^ d, w, 0, 0)
        total = lax.dynamic_update_slice(
            total, lax.dynamic_slice(total, at, (1, w, rows, cols)) - learn_rate * second[d][None], at
        )
    return (total.reshape(mats, rows, cols), new_momentum)


def orthogonal(whole):
    iterate = whole * lax.rsqrt(jnp.sum(whole * whole, axis=(1, 2), keepdims=True) + 1e-06)
    for _ in range(ITERS):
        gram = jnp.einsum("mik,mjk->mij", iterate, iterate, precision=HI)
        mix = A1 * gram + A2 * jnp.einsum("mij,mjk->mik", gram, gram, precision=HI)
        iterate = A0 * iterate + jnp.einsum("mij,mjk->mik", mix, iterate, precision=HI)
    return iterate


def plain(shards, model, grad_stack, moment_stack, weight_stack):
    new_momentum = hold_rate * moment_stack + grad_stack
    mats, rows, cols = new_momentum.shape
    x = lax.all_to_all(new_momentum, AXES, split_axis=0, concat_axis=0, tiled=True)
    x = x.reshape(shards, model, -1, rows, cols).transpose(2, 0, 3, 1, 4)
    x = orthogonal(x.reshape(-1, shards * rows, model * cols))
    x = x.reshape(-1, shards, rows, model, cols).transpose(1, 3, 0, 2, 4).reshape(mats, rows, cols)
    x = lax.all_to_all(x, AXES, split_axis=0, concat_axis=0, tiled=True)
    return ((1.0 - learn_rate * decay_rate) * weight_stack - learn_rate * x, new_momentum)


def solution(mesh):
    shards, model = mesh.shape["shard"], mesh.shape["model"]
    spec = P(None, "shard", "model")
    use = mixed if shards == 8 and model == 4 else plain
    return jax.shard_map(
        functools.partial(use, shards, model),
        mesh=mesh, in_specs=(spec,) * 3, out_specs=(spec,) * 2, check_vma=False,
    )
```

```python
import functools

import jax
import jax.numpy as jnp
from jax import lax
from jax.experimental import pallas as pl
from jax.experimental.pallas import tpu as pltpu
from jax.sharding import PartitionSpec as P


ITERS = 5
EARLY = 2
hold_rate = 0.95
learn_rate = 1.0
decay_rate = 0.1
A0, A1, A2 = 3.4445, -4.775, 2.0315
HI = lax.Precision.HIGHEST
AXES = ("shard", "model")
F32 = jnp.float32
VMEM = pl.BlockSpec(memory_space=pltpu.VMEM)


def dot(a, b):
    return lax.dot_general(a, b, (((1,), (0,)), ((), ())), precision=HI, preferred_element_type=F32)


def eye_of(n):
    i = lax.broadcasted_iota(jnp.int32, (n, n), 0)
    j = lax.broadcasted_iota(jnp.int32, (n, n), 1)
    return (i == j).astype(F32)


def chain(grams, steps, eye):
    totals = None
    for step in range(steps):
        squares = [dot(g, g) for g in grams]
        ps = [A0 * eye + A1 * g + A2 * s for g, s in zip(grams, squares)]
        if step < steps - 1:
            halves = [dot(p, g) for p, g in zip(ps, grams)]
        totals = ps if totals is None else [dot(p, t) for p, t in zip(ps, totals)]
        if step < steps - 1:
            grams = [dot(h, p) for h, p in zip(halves, ps)]
    return totals


def inverse_norm(gram, eye):
    return lax.rsqrt(jnp.sum(gram * eye, axis=(0, 1), keepdims=True) + 1e-06)


def parts3(x):
    h = x.astype(jnp.bfloat16)
    rest = x - h.astype(F32)
    m = rest.astype(jnp.bfloat16)
    return h, m, (rest - m.astype(F32)).astype(jnp.bfloat16)


def bdot(a, b):
    return lax.dot_general(a, b, (((1,), (0,)), ((), ())), preferred_element_type=F32)


def bdot_t(a, b):
    return lax.dot_general(a, b, (((1,), (1,)), ((), ())), preferred_element_type=F32)


def left_of(q):
    h, m, l = parts3(q)
    return jnp.concatenate([h, m], axis=1), jnp.concatenate([l, h], axis=1), jnp.concatenate([m, h], axis=1)


def times(left, x):
    h, m, l = x
    first, second, third = left
    return (bdot(second, jnp.concatenate([h, l], axis=0)) + bdot(third, jnp.concatenate([m, m], axis=0))) + bdot(
        first, jnp.concatenate([h, h], axis=0))


def gram_parts(x):
    h, m, l = x
    return bdot_t(h, h) + bdot_t(m, m), bdot_t(jnp.concatenate([h, h], axis=1), jnp.concatenate([m, l], axis=1))


def whole_kernel(shards, model, rows, cols, x_ref, o_ref, a_ref):
    side = shards * rows
    eye = eye_of(side)
    zero = jnp.zeros(eye.shape, F32)

    def add(totals, x):
        return tuple(t + p for t, p in zip(totals, gram_parts(x)))

    def store(at, x):
        for k in range(3):
            a_ref[k, :, at] = x[k]

    totals = (zero, zero)
    for m in range(model):
        x = parts3(jnp.concatenate([x_ref[s * model + m] for s in range(shards)], axis=0))
        store(slice(m * cols, (m + 1) * cols), x)
        totals = add(totals, x)
    g = totals[0] + (totals[1] + totals[1].T)
    norm = inverse_norm(g, eye)
    left = left_of(chain([g * (norm * norm)], EARLY, eye)[0] * norm)

    totals = (zero, zero)
    for m in range(model):
        at = slice(m * cols, (m + 1) * cols)
        x = parts3(times(left, tuple(a_ref[k, :, at] for k in range(3))))
        store(at, x)
        totals = add(totals, x)
    g = totals[0] + (totals[1] + totals[1].T)
    left = left_of(chain([g], ITERS - EARLY, eye)[0])

    for m in range(model):
        at = slice(m * cols, (m + 1) * cols)
        y = times(left, tuple(a_ref[k, :, at] for k in range(3)))
        for s in range(shards):
            o_ref[s * model + m] = y[s * rows:(s + 1) * rows]


def whole(x, shards, model):
    _, rows, cols = x.shape
    flops = 8 * (shards * rows) ** 2 * model * cols * 6
    return pl.pallas_call(
        functools.partial(whole_kernel, shards, model, rows, cols),
        out_shape=jax.ShapeDtypeStruct(x.shape, F32),
        in_specs=[VMEM],
        out_specs=VMEM,
        scratch_shapes=[pltpu.VMEM((3, shards * rows, model * cols), jnp.bfloat16)],
        cost_estimate=pl.CostEstimate(flops=flops, bytes_accessed=8 * x.size, transcendentals=0),
    )(x)


def mm(a, b):
    return jnp.einsum("mij,mjk->mik", a, b, precision=HI)


def gram_of(x):
    return jnp.einsum("mik,mjk->mij", x, x, precision=HI)


def stacked_chain(g, steps, eye):
    total = None
    for step in range(steps):
        p = A0 * eye + A1 * g + A2 * mm(g, g)
        total = p if total is None else mm(p, total)
        if step < steps - 1:
            g = mm(mm(p, g), p)
    return total


def swap(x, axis, size, bits):
    return lax.ppermute(x, axis, [(i, i ^ bits) for i in range(size)])


def summed(g, model):
    half = g.shape[0] // 2
    bit = lax.axis_index("model") % 2
    own = lax.dynamic_slice_in_dim(g, bit * half, half, 0)
    send = lax.dynamic_slice_in_dim(g, (1 - bit) * half, half, 0)
    own = own + swap(send, "model", model, 1)
    return own + swap(own, "model", model, 2)


def joined(own, model):
    bit = lax.axis_index("model") % 2
    other = swap(own, "model", model, 1)
    return jnp.where(bit == 0, jnp.concatenate([own, other]), jnp.concatenate([other, own]))


def spread(x, model):
    eye = lax.optimization_barrier(jnp.eye(x.shape[1], dtype=F32))
    g = gram_of(x)
    g = summed(g, model)
    r = lax.rsqrt(jnp.einsum("mii->m", g) + 1e-06)[:, None, None]
    q = stacked_chain(g * (r * r), EARLY, eye) * r
    x = mm(joined(q, model), x)
    g = summed(gram_of(x), model)
    q = joined(stacked_chain(g, ITERS - EARLY, eye), model)
    return mm(q, x)


def direct(blocks, shards):
    return [blocks[0]] + [swap(blocks[d], "shard", shards, d) for d in range(1, shards)]


def mixed(shards, model, grad_stack, moment_stack, weight_stack):
    mats, rows, cols = grad_stack.shape
    each = mats // shards
    w = each // 2
    me = lax.axis_index("shard")
    cut = (shards, each, rows, cols)
    first = hold_rate * moment_stack.reshape(cut)[:, :w] + grad_stack.reshape(cut)[:, :w]
    first, grad_stack = lax.optimization_barrier((first, grad_stack))
    new_momentum = hold_rate * moment_stack + grad_stack
    split = new_momentum.reshape(cut)
    first = lax.all_to_all(first.reshape(shards * model, rows, cols), AXES, split_axis=0, concat_axis=0, tiled=True)
    second = [lax.dynamic_slice(split, (me ^ d, w, 0, 0), (1, w, rows, cols))[0] for d in range(shards)]
    second = direct(second, shards)

    first = whole(first, shards, model)
    first = lax.all_to_all(first, AXES, split_axis=0, concat_axis=0, tiled=True)

    x = jnp.concatenate([b[None] for b in second], axis=0).transpose(1, 0, 2, 3)
    x = spread(x.reshape(w, shards * rows, cols), model).reshape(w, shards, rows, cols)
    second = [x[:, d] for d in range(shards)]
    second = direct(second, shards)

    kept = (1.0 - learn_rate * decay_rate) * weight_stack.reshape(cut)
    total = kept.at[:, :w].add(-learn_rate * first.reshape(shards, w, rows, cols))
    for d in range(shards):
        at = (me ^ d, w, 0, 0)
        total = lax.dynamic_update_slice(
            total, lax.dynamic_slice(total, at, (1, w, rows, cols)) - learn_rate * second[d][None], at
        )
    return (total.reshape(mats, rows, cols), new_momentum)


def orthogonal(whole):
    iterate = whole * lax.rsqrt(jnp.sum(whole * whole, axis=(1, 2), keepdims=True) + 1e-06)
    for _ in range(ITERS):
        gram = jnp.einsum("mik,mjk->mij", iterate, iterate, precision=HI)
        mix = A1 * gram + A2 * jnp.einsum("mij,mjk->mik", gram, gram, precision=HI)
        iterate = A0 * iterate + jnp.einsum("mij,mjk->mik", mix, iterate, precision=HI)
    return iterate


def plain(shards, model, grad_stack, moment_stack, weight_stack):
    new_momentum = hold_rate * moment_stack + grad_stack
    mats, rows, cols = new_momentum.shape
    x = lax.all_to_all(new_momentum, AXES, split_axis=0, concat_axis=0, tiled=True)
    x = x.reshape(shards, model, -1, rows, cols).transpose(2, 0, 3, 1, 4)
    x = orthogonal(x.reshape(-1, shards * rows, model * cols))
    x = x.reshape(-1, shards, rows, model, cols).transpose(1, 3, 0, 2, 4).reshape(mats, rows, cols)
    x = lax.all_to_all(x, AXES, split_axis=0, concat_axis=0, tiled=True)
    return ((1.0 - learn_rate * decay_rate) * weight_stack - learn_rate * x, new_momentum)


def solution(mesh):
    shards, model = mesh.shape["shard"], mesh.shape["model"]
    spec = P(None, "shard", "model")
    use = mixed if shards == 8 and model == 4 else plain
    return jax.shard_map(
        functools.partial(use, shards, model),
        mesh=mesh, in_specs=(spec,) * 3, out_specs=(spec,) * 2, check_vma=False,
    )
```

```python
import functools

import jax
import jax.numpy as jnp
from jax import lax
from jax.experimental import pallas as pl
from jax.experimental.pallas import tpu as pltpu
from jax.sharding import PartitionSpec as P


ITERS = 5
EARLY = 2
hold_rate = 0.95
learn_rate = 1.0
decay_rate = 0.1
A0, A1, A2 = 3.4445, -4.775, 2.0315
HI = lax.Precision.HIGHEST
AXES = ("shard", "model")
F32 = jnp.float32
VMEM = pl.BlockSpec(memory_space=pltpu.VMEM)


def dot(a, b):
    return lax.dot_general(a, b, (((1,), (0,)), ((), ())), precision=HI, preferred_element_type=F32)


def eye_of(n):
    i = lax.broadcasted_iota(jnp.int32, (n, n), 0)
    j = lax.broadcasted_iota(jnp.int32, (n, n), 1)
    return (i == j).astype(F32)


def chain(grams, steps, eye):
    totals = None
    for step in range(steps):
        squares = [dot(g, g) for g in grams]
        ps = [A0 * eye + A1 * g + A2 * s for g, s in zip(grams, squares)]
        if step < steps - 1:
            halves = [dot(p, g) for p, g in zip(ps, grams)]
        totals = ps if totals is None else [dot(p, t) for p, t in zip(ps, totals)]
        if step < steps - 1:
            grams = [dot(h, p) for h, p in zip(halves, ps)]
    return totals


def inverse_norm(gram, eye):
    return lax.rsqrt(jnp.sum(gram * eye, axis=(0, 1), keepdims=True) + 1e-06)


def parts3(x):
    h = x.astype(jnp.bfloat16)
    rest = x - h.astype(F32)
    m = rest.astype(jnp.bfloat16)
    return h, m, (rest - m.astype(F32)).astype(jnp.bfloat16)


def bdot(a, b):
    return lax.dot_general(a, b, (((1,), (0,)), ((), ())), preferred_element_type=F32)


def bdot_t(a, b):
    return lax.dot_general(a, b, (((1,), (1,)), ((), ())), preferred_element_type=F32)


def left_of(q):
    h, m, l = parts3(q)
    return jnp.concatenate([h, m], axis=1), jnp.concatenate([l, h], axis=1), jnp.concatenate([m, h], axis=1)


def times(left, x):
    h, m, l = x
    first, second, third = left
    return (bdot(second, jnp.concatenate([h, l], axis=0)) + bdot(third, jnp.concatenate([m, m], axis=0))) + bdot(
        first, jnp.concatenate([h, h], axis=0))


def gram_parts(x):
    h, m, l = x
    return bdot_t(h, h) + bdot_t(m, m), bdot_t(jnp.concatenate([h, h], axis=1), jnp.concatenate([m, l], axis=1))


def whole_kernel(shards, model, rows, cols, x_ref, o_ref, a_ref):
    side = shards * rows
    eye = eye_of(side)
    zero = jnp.zeros(eye.shape, F32)

    def add(totals, x):
        return tuple(t + p for t, p in zip(totals, gram_parts(x)))

    def store(at, x):
        for k in range(3):
            a_ref[k, :, at] = x[k]

    totals = (zero, zero)
    for m in range(model):
        x = parts3(jnp.concatenate([x_ref[s * model + m] for s in range(shards)], axis=0))
        store(slice(m * cols, (m + 1) * cols), x)
        totals = add(totals, x)
    g = totals[0] + (totals[1] + totals[1].T)
    norm = inverse_norm(g, eye)
    left = left_of(chain([g * (norm * norm)], EARLY, eye)[0] * norm)

    totals = (zero, zero)
    for m in range(model):
        at = slice(m * cols, (m + 1) * cols)
        x = parts3(times(left, tuple(a_ref[k, :, at] for k in range(3))))
        store(at, x)
        totals = add(totals, x)
    g = totals[0] + (totals[1] + totals[1].T)
    left = left_of(chain([g], ITERS - EARLY, eye)[0])

    for m in range(model):
        at = slice(m * cols, (m + 1) * cols)
        y = times(left, tuple(a_ref[k, :, at] for k in range(3)))
        for s in range(shards):
            o_ref[s * model + m] = y[s * rows:(s + 1) * rows]


def whole(x, shards, model):
    _, rows, cols = x.shape
    flops = 8 * (shards * rows) ** 2 * model * cols * 6
    return pl.pallas_call(
        functools.partial(whole_kernel, shards, model, rows, cols),
        out_shape=jax.ShapeDtypeStruct(x.shape, F32),
        in_specs=[VMEM],
        out_specs=VMEM,
        scratch_shapes=[pltpu.VMEM((3, shards * rows, model * cols), jnp.bfloat16)],
        cost_estimate=pl.CostEstimate(flops=flops, bytes_accessed=8 * x.size, transcendentals=0),
    )(x)


def mm(a, b):
    return jnp.einsum("mij,mjk->mik", a, b, precision=HI)


def gram_of(x):
    return jnp.einsum("mik,mjk->mij", x, x, precision=HI)


def stacked_chain(g, steps, eye):
    total = None
    for step in range(steps):
        p = A0 * eye + A1 * g + A2 * mm(g, g)
        total = p if total is None else mm(p, total)
        if step < steps - 1:
            g = mm(mm(p, g), p)
    return total


def swap(x, axis, size, bits):
    return lax.ppermute(x, axis, [(i, i ^ bits) for i in range(size)])


def summed(g, model):
    half = g.shape[0] // 2
    bit = lax.axis_index("model") % 2
    own = lax.dynamic_slice_in_dim(g, bit * half, half, 0)
    send = lax.dynamic_slice_in_dim(g, (1 - bit) * half, half, 0)
    own = own + swap(send, "model", model, 1)
    if half % 2:
        return own + swap(own, "model", model, 2)
    a, b = own[: half // 2], own[half // 2 :]
    side = own.shape[1]
    i = lax.broadcasted_iota(jnp.int32, (side, side), 0)
    j = lax.broadcasted_iota(jnp.int32, (side, side), 1)
    diagonal = jnp.einsum("mii->mi", b)[:, None, :]
    pair = jnp.concatenate([jnp.where(i <= j, a, b), jnp.broadcast_to(diagonal, (half // 2, 8, side))], axis=1)
    pair = swap(pair, "model", model, 2)
    pair, diagonal = pair[:, :side], pair[:, side]
    turned = pair.transpose(0, 2, 1)
    a = a + jnp.where(i <= j, pair, turned)
    b = b + jnp.where(i == j, diagonal[:, None, :], jnp.where(i > j, pair, turned))
    return jnp.concatenate([a, b])


def joined(own, model):
    bit = lax.axis_index("model") % 2
    other = swap(own, "model", model, 1)
    return jnp.where(bit == 0, jnp.concatenate([own, other]), jnp.concatenate([other, own]))


def spread(x, model):
    eye = lax.optimization_barrier(jnp.eye(x.shape[1], dtype=F32))
    g = gram_of(x)
    g = summed(g, model)
    r = lax.rsqrt(jnp.einsum("mii->m", g) + 1e-06)[:, None, None]
    q = stacked_chain(g * (r * r), EARLY, eye) * r
    x = mm(joined(q, model), x)
    g = summed(gram_of(x), model)
    q = joined(stacked_chain(g, ITERS - EARLY, eye), model)
    return jnp.einsum("mij,mjk->mik", q, x, precision=lax.Precision.HIGH)


def direct(blocks, shards):
    return [blocks[0]] + [swap(blocks[d], "shard", shards, d) for d in range(1, shards)]


def mixed(shards, model, grad_stack, moment_stack, weight_stack):
    mats, rows, cols = grad_stack.shape
    each = mats // shards
    w = each // 2
    me = lax.axis_index("shard")
    cut = (shards, each, rows, cols)
    first = hold_rate * moment_stack.reshape(cut)[:, :w] + grad_stack.reshape(cut)[:, :w]
    first, grad_stack = lax.optimization_barrier((first, grad_stack))
    new_momentum = hold_rate * moment_stack + grad_stack
    split = new_momentum.reshape(cut)
    first = lax.all_to_all(first.reshape(shards * model, rows, cols), AXES, split_axis=0, concat_axis=0, tiled=True)
    second = [lax.dynamic_slice(split, (me ^ d, w, 0, 0), (1, w, rows, cols))[0] for d in range(shards)]
    second = direct(second, shards)

    first = whole(first, shards, model)
    first = lax.all_to_all(first, AXES, split_axis=0, concat_axis=0, tiled=True)

    x = jnp.concatenate([b[None] for b in second], axis=0).transpose(1, 0, 2, 3)
    x = spread(x.reshape(w, shards * rows, cols), model).reshape(w, shards, rows, cols)
    second = [x[:, d] for d in range(shards)]
    second = direct(second, shards)

    kept = (1.0 - learn_rate * decay_rate) * weight_stack.reshape(cut)
    total = kept.at[:, :w].add(-learn_rate * first.reshape(shards, w, rows, cols))
    for d in range(shards):
        at = (me ^ d, w, 0, 0)
        total = lax.dynamic_update_slice(
            total, lax.dynamic_slice(total, at, (1, w, rows, cols)) - learn_rate * second[d][None], at
        )
    return (total.reshape(mats, rows, cols), new_momentum)


def orthogonal(whole):
    iterate = whole * lax.rsqrt(jnp.sum(whole * whole, axis=(1, 2), keepdims=True) + 1e-06)
    for _ in range(ITERS):
        gram = jnp.einsum("mik,mjk->mij", iterate, iterate, precision=HI)
        mix = A1 * gram + A2 * jnp.einsum("mij,mjk->mik", gram, gram, precision=HI)
        iterate = A0 * iterate + jnp.einsum("mij,mjk->mik", mix, iterate, precision=HI)
    return iterate


def plain(shards, model, grad_stack, moment_stack, weight_stack):
    new_momentum = hold_rate * moment_stack + grad_stack
    mats, rows, cols = new_momentum.shape
    x = lax.all_to_all(new_momentum, AXES, split_axis=0, concat_axis=0, tiled=True)
    x = x.reshape(shards, model, -1, rows, cols).transpose(2, 0, 3, 1, 4)
    x = orthogonal(x.reshape(-1, shards * rows, model * cols))
    x = x.reshape(-1, shards, rows, model, cols).transpose(1, 3, 0, 2, 4).reshape(mats, rows, cols)
    x = lax.all_to_all(x, AXES, split_axis=0, concat_axis=0, tiled=True)
    return ((1.0 - learn_rate * decay_rate) * weight_stack - learn_rate * x, new_momentum)


def solution(mesh):
    shards, model = mesh.shape["shard"], mesh.shape["model"]
    spec = P(None, "shard", "model")
    use = mixed if shards == 8 and model == 4 else plain
    return jax.shard_map(
        functools.partial(use, shards, model),
        mesh=mesh, in_specs=(spec,) * 3, out_specs=(spec,) * 2, check_vma=False,
    )
```
